32 devices in a mesh: grp: 2 (over x), tok: 8 (over z, y), side: 2 (over core).
Axes of the slice: x: 2, y: 2, z: 4, core: 2. Of those that a mesh axis runs over, the one named last changes fastest.
Arguments:
- hidden_in: bfloat16 [512, 3072], P(('grp', 'tok')), parts along dimension 0, may hold values from -6 to 6
- queries: bfloat16 [512, 24, 128], P(('grp', 'tok'), 'side'), parts along dimension 0, may hold values from -32 to 32
- key_new: bfloat16 [512, 4, 128], P(('grp', 'tok'), 'side'), parts along dimension 0, may hold values from -32 to 32
- value_new: bfloat16 [512, 4, 128], P(('grp', 'tok'), 'side'), parts along dimension 0, may hold values from -6 to 6
- cache_keys: bfloat16 [512, 4, 128, 128], P(('grp', 'tok'), 'side'), parts along dimension 0, may hold values from -32 to 32
- cache_values: bfloat16 [512, 4, 128, 128], P(('grp', 'tok'), 'side'), parts along dimension 0, may hold values from -6 to 6
- lengths: int32 [512], P(('grp', 'tok')), parts along dimension 0, may hold values from 1 to 128, 16384 in all
- out_weight: bfloat16 [3072, 3072], P('side', 'tok'), may hold values from -0.109375 to 0.109375
- norm_gain: float32 [3072], replicated, may hold values from 0.1 to 1.9
- router_weight: float32 [3072, 4], replicated, may hold values from -0.109375 to 0.109375
- gate_weight: bfloat16 [3072, 32768], P(None, ('tok', 'side')), may hold values from -0.109375 to 0.109375
- up_weight: bfloat16 [3072, 32768], P(None, ('tok', 'side')), may hold values from -0.109375 to 0.109375
- down_weight: bfloat16 [32768, 3072], P(('tok', 'side')), may hold values from -0.0625 to 0.0625
- routes: int32 [512, 2], P('grp'), parts along dimension 0, may hold values from 0 to 3, all different within a row; in each aligned block of 32 rows (0 to 31, 32 to 63, ...) at most 24 rows name the same one
Outputs:
- mixed: bfloat16 [512, 3072], P(('grp', 'tok')), parts along dimension 0
The draws below stay inside these ranges and needn't reach their ends.
There are 2 independent parts, one for each index of `grp`. The reference program is written for one: setup_inputs(seed, part) draws one part's arguments, and reference() takes and returns one part's arrays. A program takes and returns all parts, laid end to end along the dimension named above; an argument that names none is the same for every part. Nothing has to cross between parts.
Inputs may be any that keep to these rules, and one draw needn't show every extreme that they name: Every sequence has at least one valid cache position and some sequence has 128; in each serving group the lengths sum to 16384. `routes`: each row names two different experts; among the rows of one index of tok (aligned blocks of 32 rows) no expert is named by more than 24 rows, and some expert reaches 24 in some block.
All inputs are finite; a program needn't handle non-finite values.
Results may differ from the reference program's by a relative error of at most 0.0075.
Values may be sent and summed in bfloat16 or wider, within the bound.
No kernel may reach another device: no remote copies, remote signals or barrier semaphores. Data moves between devices by JAX's collectives and lax.ppermute only.
A program may use at most 128 MiB of HBM per device.

```python
import math
import jax
import jax.numpy as jnp
import numpy as np
from jax import lax

D = 3072
HEADS = 24
KV_HEADS = 4
HD = 128
EXPERTS = 4
HID = 8192
TOP = 2
SEQ_DEV = 32
L_MAX = 128
CAP = 24
SEQS = 256


def draw_queries(key, part):
    sampled = jnp.clip(jax.random.normal(jax.random.fold_in(key, 11), (SEQS, HEADS, HD), jnp.float32), -6.0, 6.0)
    return sampled.astype(jnp.bfloat16)


def draw_key_new(key, part):
    sampled = jnp.clip(jax.random.normal(jax.random.fold_in(key, 23), (SEQS, KV_HEADS, HD), jnp.float32), -6.0, 6.0)
    return sampled.astype(jnp.bfloat16)


def draw_cache_keys(key, part):
    sampled = jnp.clip(jax.random.normal(jax.random.fold_in(key, 37), (SEQS, KV_HEADS, L_MAX, HD), jnp.float32), -6.0, 6.0)
    return sampled.astype(jnp.bfloat16)


def steps_of(own_key, extent, pieces, least, top_value):
    factor_of, own = 1.0, jax.random.fold_in(own_key, 6)
    for dim, parts in pieces:
        heights = jnp.exp(jax.random.uniform(jax.random.fold_in(own, dim), (parts,), jnp.float32, least / len(pieces), top_value / len(pieces)))
        factor_of = factor_of * jnp.repeat(heights, extent[dim] // parts).reshape([-1 if axis == dim else 1 for axis in range(len(extent))])
    return factor_of


def profile(number_of, total, limit, slope):
    weights = [(1 << 20) // math.isqrt(standing ** slope) + 1 for standing in range(2, number_of + 1)]
    rest, counts = total - limit - (number_of - 1), [1] * (number_of - 1)
    while rest > 0:
        candidates = [i for i in range(number_of - 1) if counts[i] < limit]
        pool, budget = sum([weights[i] for i in candidates]), rest
        for i in candidates:
            extra = min(limit - counts[i], max(1, budget * weights[i] // pool), rest)
            counts[i] = counts[i] + extra
            rest = rest - extra
    return np.array([limit] + counts)


def ragged_sizes(own_key, number_of, total, most, skew):
    if number_of == 2:
        one = jax.random.randint(own_key, (), max(1, total - most), min(most, total - 1) + 1)
        return jnp.stack([one, total - one])
    sizes = jnp.asarray(profile(number_of, total, most, skew), jnp.int32)
    pairs = (number_of - 1) // 2
    source_of, taker = sizes[1:1 + 2 * pairs:2], sizes[2:2 + 2 * pairs:2]
    room = jnp.minimum(source_of - 1, most - taker)
    passed = jax.random.randint(jax.random.fold_in(own_key, 1), (pairs,), 0, 1 << 20) % (room + 1)
    sizes = sizes.at[1:1 + 2 * pairs:2].set(source_of - passed).at[2:2 + 2 * pairs:2].set(taker + passed)
    return sizes[jax.random.permutation(jax.random.fold_in(own_key, 2), number_of)]


def shared_out(own_key, own, number, rows, amount, top, bound, skew):
    ranking = jax.random.permutation(own_key, amount)
    heavy_load, usual = portions_of(amount, rows * top, bound, skew, True), portions_of(amount, rows * top, bound, skew, False)
    places = jnp.arange(amount)

    def named(sizes, turn):
        used = int((sizes > 0).sum())
        fixed = max(1, used // 4)
        moved = fixed + (places - fixed + turn * (used - fixed)) % max(1, amount - fixed)
        return jnp.zeros((amount,), jnp.int32).at[ranking[jnp.where(places < fixed, places, moved)]].set(jnp.asarray(sizes, jnp.int32))

    sizes = jnp.where(number % 4 == 0, named(heavy_load, number // 4), named(usual, number - number // 4 - 1))
    mixed = jax.random.permutation(jax.random.fold_in(own, 3), amount)
    source_of, sink = mixed[0:amount // 2 * 2:2], mixed[1:amount // 2 * 2:2]
    slack = jnp.minimum(sizes[source_of] - 1, bound - sizes[sink]) // 2
    slack = jnp.where((source_of == ranking[0]) | (sink == ranking[0]) | (sizes[sink] == 0), 0, jnp.maximum(slack, 0))
    moved = jax.random.randint(jax.random.fold_in(own, 4), (amount // 2,), 0, 1 << 20) % (slack + 1)
    sizes = sizes.at[source_of].add(-moved).at[sink].add(moved)
    labels = jnp.searchsorted(jnp.cumsum(sizes), jnp.arange(rows * top), side="right").astype(jnp.int32)
    table = labels.reshape(top, rows).T
    table = table[jax.random.permutation(jax.random.fold_in(own, 1), rows)]
    turn = jax.random.randint(jax.random.fold_in(own, 2), (rows, 1), 0, top)
    return jnp.take_along_axis(table, (jnp.arange(top)[None, :] + turn) % top, axis=1)


def portions_of(number_of, total, bound, slope, full):
    portions = [(1 << 20) // math.isqrt(standing ** slope) + 1 for standing in range(1, number_of + 1)]
    largest = bound if full else min(bound, max(-(-total // number_of), total * portions[0] // sum(portions)))
    least = 1 if total - largest >= number_of - 1 else 0
    counts, surplus = [largest] + [least] * (number_of - 1), total - largest - least * (number_of - 1)
    while surplus > 0:
        movable = [i for i in range(1, number_of) if counts[i] < largest] or [i for i in range(1, number_of) if counts[i] < bound]
        whole, budget = sum([portions[i] for i in movable]), surplus
        for i in movable:
            extra = min(bound - counts[i], max(1, budget * portions[i] // whole), surplus)
            counts[i] = counts[i] + extra
            surplus = surplus - extra
    return np.array(counts)


def noise(own_key, shape, scale, limit, cuts=(), kind=jnp.bfloat16):
    array = jax.random.normal(own_key, shape, jnp.float32) * scale
    if len(cuts) > 0:
        array = steps_of(own_key, shape, cuts, -0.22, 0.18) * array
    return jnp.clip(array, min=-limit, max=limit).astype(kind)


def setup_inputs(seed: int = 0, part: int = 0) -> dict:
    key_of = jax.random.split(jax.random.key(seed), 15)
    part_keys = jax.random.split(jax.random.fold_in(key_of[14], part), 15)
    hidden_in = noise(part_keys[0], (SEQS, D), 1.0, 6.0, ((0, 8),))
    queries = draw_queries(jax.random.fold_in(jax.random.fold_in(key_of[14], part), 71), part)
    key_new = draw_key_new(jax.random.fold_in(jax.random.fold_in(key_of[14], part), 71), part)
    value_new = noise(part_keys[3], (SEQS, KV_HEADS, HD), 1.0, 6.0, ((0, 8), (1, 2)))
    cache_keys = draw_cache_keys(jax.random.fold_in(jax.random.fold_in(key_of[14], part), 71), part)
    cache_values = noise(part_keys[5], (SEQS, KV_HEADS, L_MAX, HD), 1.0, 6.0, ((0, 8), (1, 2)))
    lengths = ragged_sizes(part_keys[6], SEQS, SEQS * L_MAX // 2, L_MAX, 2).astype(jnp.int32)
    out_weight = noise(key_of[7], (HEADS * HD, D), (HEADS * HD) ** -0.5, 0.109375, ((0, 2), (1, 8)))
    norm_gain = jnp.clip(1.0 + 0.18 * jax.random.normal(key_of[8], (D,), jnp.float32), 0.1, 1.9)
    router_weight = noise(key_of[9], (D, EXPERTS), D ** -0.5, 0.109375, (), jnp.float32)
    gate_weight = noise(key_of[10], (D, EXPERTS * HID), D ** -0.5, 0.109375, ((1, 16),))
    up_weight = noise(key_of[11], (D, EXPERTS * HID), D ** -0.5, 0.109375, ((1, 16),))
    down_weight = noise(key_of[12], (EXPERTS * HID, D), HID ** -0.5, 0.0625, ((0, 16),))
    routes_keys = jax.random.split(jax.random.fold_in(part_keys[13], 1), SEQS // SEQ_DEV)
    routes_turns = jax.random.permutation(jax.random.fold_in(part_keys[13], 3), SEQS // SEQ_DEV)
    routes = jax.vmap(lambda own, number: shared_out(jax.random.fold_in(part_keys[13], 2), own, number, SEQ_DEV, EXPERTS, TOP, CAP, 2))(routes_keys, routes_turns).reshape((SEQS, TOP))
    return dict(hidden_in=hidden_in, queries=queries, key_new=key_new, value_new=value_new, cache_keys=cache_keys, cache_values=cache_values, lengths=lengths, out_weight=out_weight, norm_gain=norm_gain, router_weight=router_weight, gate_weight=gate_weight, up_weight=up_weight, down_weight=down_weight, routes=routes)


def reference(hidden_in, queries, key_new, value_new, cache_keys, cache_values, lengths, out_weight, norm_gain, router_weight, gate_weight, up_weight, down_weight, routes):
    group_size = HEADS // KV_HEADS
    scaling = 1.0 / math.sqrt(HD)
    grouped = queries.astype(jnp.float32).reshape(SEQS, KV_HEADS, group_size, HD)
    scores = jnp.einsum('skgd,skpd->skgp', grouped, cache_keys.astype(jnp.float32)) * scaling
    usable = jnp.arange(L_MAX, dtype=jnp.int32)[None, :] < lengths[:, None]
    scores = jnp.where(usable[:, None, None, :], scores, -jnp.inf)
    own_score = jnp.einsum('skgd,skd->skg', grouped, key_new.astype(jnp.float32)) * scaling
    top_score = jnp.maximum(lax.optimization_barrier(jnp.max(scores, axis=-1)), own_score)
    weights = jnp.exp(scores - top_score[..., None])
    own_weight = jnp.exp(own_score - top_score)
    totals = lax.optimization_barrier(jnp.sum(weights, axis=-1)) + own_weight
    prob_low = (weights / totals[..., None]).astype(jnp.bfloat16)
    own_low = (own_weight / totals).astype(jnp.bfloat16)
    mixture = jnp.einsum('skgp,skpd->skgd', prob_low.astype(jnp.float32), cache_values.astype(jnp.float32))
    mixture = mixture + own_low.astype(jnp.float32)[..., None] * value_new.astype(jnp.float32)[:, :, None, :]
    attn_out = mixture.astype(jnp.bfloat16).reshape(SEQS, HEADS * HD)
    projected = jnp.dot(attn_out, out_weight, preferred_element_type=jnp.float32)
    residual = (hidden_in.astype(jnp.float32) + projected).astype(jnp.bfloat16)
    stream = residual.astype(jnp.float32)
    normed = (stream * lax.rsqrt(lax.optimization_barrier(jnp.mean(stream * stream, axis=-1, keepdims=True)) + 1e-05) * norm_gain).astype(jnp.bfloat16)
    logits = jnp.dot(normed.astype(jnp.float32), router_weight, precision=lax.Precision.HIGHEST)
    expert_ids = jnp.arange(EXPERTS, dtype=jnp.int32)
    picks = (routes[:, :, None] == expert_ids[None, None, :]).astype(jnp.float32)
    chosen_logits = lax.optimization_barrier(jnp.sum(picks * logits[:, None, :], axis=-1))
    leading = jax.nn.sigmoid(chosen_logits[:, 0] - chosen_logits[:, 1])
    gates = jnp.stack([leading, 1.0 - leading], axis=1)
    coefficient = lax.optimization_barrier(jnp.sum(gates[:, :, None] * picks, axis=1))

    def one_expert(index):
        gate_cols = lax.dynamic_slice_in_dim(gate_weight, index * HID, HID, 1)
        up_cols = lax.dynamic_slice_in_dim(up_weight, index * HID, HID, 1)
        down_rows = lax.dynamic_slice_in_dim(down_weight, index * HID, HID, 0)
        gated = jnp.dot(normed, gate_cols, preferred_element_type=jnp.float32)
        upward = jnp.dot(normed, up_cols, preferred_element_type=jnp.float32)
        active = (jax.nn.silu(gated) * upward).astype(jnp.bfloat16)
        return jnp.dot(active, down_rows, preferred_element_type=jnp.float32)
    outputs = lax.map(one_expert, expert_ids)
    combined = lax.optimization_barrier(jnp.sum(coefficient.T[:, :, None] * outputs, axis=0))
    return (stream + combined).astype(jnp.bfloat16)
```

```python
import math

import jax
import jax.numpy as jnp
from jax import lax
from jax.sharding import PartitionSpec as P


def attend(queries, key_new, value_new, cache_keys, cache_values, lengths):
    seq_count, head_count, head_width = queries.shape
    kv_count = key_new.shape[1]
    places = cache_keys.shape[2]
    scaling = 1.0 / math.sqrt(head_width)
    grouped = queries.reshape(seq_count, kv_count, head_count // kv_count, head_width)
    scores = (
        jnp.einsum("skgd,skpd->skgp", grouped, cache_keys, preferred_element_type=jnp.float32)
        * scaling
    )
    usable = jnp.arange(places, dtype=jnp.int32)[None, :] < lengths[:, None]
    scores = jnp.where(usable[:, None, None, :], scores, -jnp.inf)
    own_score = (
        jnp.einsum("skgd,skd->skg", grouped, key_new, preferred_element_type=jnp.float32) * scaling
    )
    top_score = jnp.maximum(jnp.max(scores, axis=-1), own_score)
    weights = jnp.exp(scores - top_score[..., None])
    own_weight = jnp.exp(own_score - top_score)
    totals = jnp.sum(weights, axis=-1) + own_weight
    prob_low = (weights / totals[..., None]).astype(jnp.bfloat16)
    own_low = (own_weight / totals).astype(jnp.bfloat16)
    mixture = jnp.einsum(
        "skgp,skpd->skgd", prob_low, cache_values, preferred_element_type=jnp.float32
    )
    mixture = (
        mixture
        + own_low.astype(jnp.float32)[..., None] * value_new.astype(jnp.float32)[:, :, None, :]
    )
    return mixture.astype(jnp.bfloat16).reshape(seq_count, head_count * head_width)


def coefficients(normed, routes, router_weight):
    logits = jnp.dot(normed.astype(jnp.float32), router_weight, precision=lax.Precision.HIGHEST)
    expert_ids = jnp.arange(router_weight.shape[1], dtype=jnp.int32)
    picks = (routes[:, :, None] == expert_ids[None, None, :]).astype(jnp.float32)
    chosen = jnp.sum(picks * logits[:, None, :], axis=-1)
    leading = jax.nn.sigmoid(chosen[:, 0] - chosen[:, 1])
    gates = jnp.stack([leading, 1.0 - leading], axis=1)
    return jnp.sum(gates[:, :, None] * picks, axis=1)


def pick(stack, index):
    return lax.dynamic_index_in_dim(stack, index, 0, keepdims=False)


def local(
    hidden_in,
    queries,
    key_new,
    value_new,
    cache_keys,
    cache_values,
    lengths,
    out_weight,
    norm_gain,
    router_weight,
    gate_weight,
    up_weight,
    down_weight,
    routes,
):
    rows, width = hidden_in.shape
    toks = lax.axis_size("tok")
    sides = lax.axis_size("side")
    experts = router_weight.shape[1]
    lines = toks // 2
    half = rows // sides
    cols = out_weight.shape[1]
    span = out_weight.shape[0]
    tok = lax.axis_index("tok")
    side = lax.axis_index("side")
    first_swap = [(t, t ^ 1) for t in range(toks)]
    side_swap = [(0, 1), (1, 0)]

    def across(value):
        return lax.ppermute(value, "side", side_swap)

    def near(value):
        return lax.ppermute(value, "tok", first_swap)

    def line(value, k):
        return lax.ppermute(value, "tok", [(t, t ^ (2 * k)) for t in range(toks)])

    hidden_half = lax.dynamic_slice_in_dim(hidden_in, side * half, half, 0)

    def piece(target):
        part = lax.dynamic_slice_in_dim(hidden_half, target * cols, cols, 1)
        return jnp.concatenate([part[: half // 2], part[half // 2 :]], axis=1)

    attn_out = attend(queries, key_new, value_new, cache_keys, cache_values, lengths)
    arrived = []
    for k in range(lines):
        extra = jnp.concatenate([piece(tok ^ (2 * k)), piece(tok ^ (2 * k) ^ 1)], axis=1)
        extra = extra.reshape(half * 2 * cols // span, span)
        message = jnp.concatenate([attn_out, extra], axis=0)
        arrived.append(line(message, k) if k else message)
    mine = [m[:rows] for m in arrived]
    folded = [m[rows:].reshape(half // 2, 4 * cols) for m in arrived]
    keep = [f[:, : 2 * cols] for f in folded]
    forward = jnp.concatenate([f[:, 2 * cols :] for f in folded], axis=0)
    forward = forward.reshape(lines * half * cols // span, span)
    passed = near(jnp.concatenate(mine + [forward], axis=0))
    theirs = [passed[k * rows : (k + 1) * rows] for k in range(lines)]
    given = passed[lines * rows :].reshape(lines, half // 2, 2 * cols)
    blocks, hidden_blocks = [], []
    for k in range(lines):
        blocks += [mine[k], theirs[k]]
        for f in (keep[k], given[k]):
            hidden_blocks.append(jnp.concatenate([f[:, :cols], f[:, cols:]], axis=0))
    columns = jnp.dot(
        jnp.concatenate(blocks, axis=0), out_weight, preferred_element_type=jnp.float32
    ).reshape(toks, sides, half, cols)
    other = lax.dynamic_index_in_dim(columns, 1 - side, 1, keepdims=False)
    own = lax.dynamic_index_in_dim(columns, side, 1, keepdims=False)
    relative = (
        jnp.stack(hidden_blocks).astype(jnp.float32) + (own + across(other))
    ).astype(jnp.bfloat16)
    residual = jnp.concatenate([pick(relative, tok ^ b) for b in range(toks)], axis=0)
    parts = [residual] + [line(residual, k) for k in range(1, lines)]
    stacked = jnp.stack(parts)
    crossed = near(stacked)
    pieces = jnp.stack([stacked, crossed], axis=1).reshape(toks, toks * half, cols)
    stream = jnp.concatenate([pick(pieces, tok ^ b) for b in range(toks)], axis=1)
    wide = stream.astype(jnp.float32)
    normed = (
        wide * lax.rsqrt(jnp.mean(wide * wide, axis=-1, keepdims=True) + 1e-05) * norm_gain
    ).astype(jnp.bfloat16)
    partner = across(normed)
    own_routes = lax.dynamic_index_in_dim(
        routes.reshape(toks, sides, half, -1), side, 1, keepdims=False
    ).reshape(toks * half, -1)
    coefficient = coefficients(normed, own_routes, router_weight)
    expert = tok // (toks // experts)
    scale = lax.dynamic_slice_in_dim(coefficient, expert, 1, 1)
    block = jnp.concatenate([normed, partner], axis=0)
    gated = jnp.dot(block, gate_weight, preferred_element_type=jnp.float32)
    upward = jnp.dot(block, up_weight, preferred_element_type=jnp.float32)
    active = (jax.nn.silu(gated) * upward).astype(jnp.bfloat16)
    partial = jnp.dot(active, down_weight, preferred_element_type=jnp.float32)
    kept, sent = partial[: toks * half], partial[toks * half :]
    joined = (kept + across(sent.astype(jnp.bfloat16)).astype(jnp.float32)) * scale
    joined = joined.astype(jnp.bfloat16).reshape(lines, 2, half, width)
    y_own = lax.dynamic_index_in_dim(joined, tok % 2, 1, keepdims=False)
    y_other = lax.dynamic_index_in_dim(joined, 1 - tok % 2, 1, keepdims=False)
    pair = y_own.astype(jnp.float32) + near(y_other).astype(jnp.float32)
    level = tok // 2
    pair_low = pair.astype(jnp.bfloat16)
    total = pick(pair, level)
    for k in range(1, lines):
        total = total + line(pick(pair_low, level ^ k), k).astype(jnp.float32)
    mine_stream = lax.dynamic_slice_in_dim(wide, tok * half, half, 0)
    result = (mine_stream + total).astype(jnp.bfloat16)
    mate = across(result)
    low = jnp.where(side == 0, result, mate)
    high = jnp.where(side == 0, mate, result)
    return jnp.concatenate([low, high], axis=0)


def solution(mesh):
    return jax.shard_map(
        local,
        mesh=mesh,
        in_specs=(
            P(("grp", "tok"), None),
            P(("grp", "tok"), "side", None),
            P(("grp", "tok"), "side", None),
            P(("grp", "tok"), "side", None),
            P(("grp", "tok"), "side", None, None),
            P(("grp", "tok"), "side", None, None),
            P(("grp", "tok")),
            P("side", "tok"),
            P(),
            P(),
            P(None, ("tok", "side")),
            P(None, ("tok", "side")),
            P(("tok", "side"), None),
            P("grp", None),
        ),
        out_specs=P(("grp", "tok"), None),
        check_vma=False,
    )
```

```python
import math

import jax
import jax.numpy as jnp
from jax import lax
from jax.experimental import pallas as pl
from jax.experimental.pallas import tpu as pltpu
from jax.sharding import PartitionSpec as P


def attend(queries, key_new, value_new, cache_keys, cache_values, lengths):
    seq_count, head_count, head_width = queries.shape
    kv_count = key_new.shape[1]
    places = cache_keys.shape[2]
    scaling = 1.0 / math.sqrt(head_width)
    grouped = queries.reshape(seq_count, kv_count, head_count // kv_count, head_width)
    scores = (
        jnp.einsum("skgd,skpd->skgp", grouped, cache_keys, preferred_element_type=jnp.float32)
        * scaling
    )
    usable = jnp.arange(places, dtype=jnp.int32)[None, :] < lengths[:, None]
    scores = jnp.where(usable[:, None, None, :], scores, -jnp.inf)
    own_score = (
        jnp.einsum("skgd,skd->skg", grouped, key_new, preferred_element_type=jnp.float32) * scaling
    )
    top_score = jnp.maximum(jnp.max(scores, axis=-1), own_score)
    weights = jnp.exp(scores - top_score[..., None])
    own_weight = jnp.exp(own_score - top_score)
    totals = jnp.sum(weights, axis=-1) + own_weight
    prob_low = (weights / totals[..., None]).astype(jnp.bfloat16)
    own_low = (own_weight / totals).astype(jnp.bfloat16)
    mixture = jnp.einsum(
        "skgp,skpd->skgd", prob_low, cache_values, preferred_element_type=jnp.float32
    )
    mixture = (
        mixture
        + own_low.astype(jnp.float32)[..., None] * value_new.astype(jnp.float32)[:, :, None, :]
    )
    return mixture.astype(jnp.bfloat16).reshape(seq_count, head_count * head_width)


def coefficients(normed, routes, router_weight):
    logits = jnp.dot(normed.astype(jnp.float32), router_weight, precision=lax.Precision.HIGHEST)
    expert_ids = jnp.arange(router_weight.shape[1], dtype=jnp.int32)
    picks = (routes[:, :, None] == expert_ids[None, None, :]).astype(jnp.float32)
    chosen = jnp.sum(picks * logits[:, None, :], axis=-1)
    leading = jax.nn.sigmoid(chosen[:, 0] - chosen[:, 1])
    gates = jnp.stack([leading, 1.0 - leading], axis=1)
    return jnp.sum(gates[:, :, None] * picks, axis=1)


def experts_kernel(own, other, gate, up, down, kept, sent, block, gates, ups, active, sems):
    rows = own.shape[0]
    hidden = gate.shape[1]
    step = min(512, hidden)
    count = hidden // step

    def copies(c):
        part = pl.ds(c * step, step)
        return [
            pltpu.make_async_copy(source.at[:, part], target.at[:, part], sems.at[i, c])
            for i, (source, target) in enumerate(((gate, gates), (up, ups)))
        ]

    for c in range(count):
        for copy in copies(c):
            copy.start()
    block[:rows] = own[...]
    block[rows:] = other[...]
    for c in range(count):
        first, second = copies(c)
        at = slice(c * step, (c + 1) * step)
        first.wait()
        gated = jnp.dot(block[...], gates[:, at], preferred_element_type=jnp.float32)
        second.wait()
        upward = jnp.dot(block[...], ups[:, at], preferred_element_type=jnp.float32)
        active[:, at] = (jax.nn.silu(gated) * upward).astype(jnp.bfloat16)
    width = down.shape[1]
    for c in range(0, width, 512):
        out = jnp.dot(active[...], down[:, c : c + 512], preferred_element_type=jnp.float32)
        kept[:, c : c + 512] = out[:rows]
        sent[:, c : c + 512] = out[rows:].astype(jnp.bfloat16)


def stage(weight):
    def body(source, target):
        pltpu.sync_copy(source, target)

    return pl.pallas_call(
        body,
        in_specs=[pl.BlockSpec(memory_space=pltpu.HBM)],
        out_specs=pl.BlockSpec(memory_space=pltpu.VMEM),
        out_shape=pltpu.VMEM(weight.shape, weight.dtype),
        cost_estimate=pl.CostEstimate(
            flops=weight.size * 600, transcendentals=0, bytes_accessed=2 * weight.size
        ),
        compiler_params=pltpu.CompilerParams(vmem_limit_bytes=1 << 20),
        name="stage",
    )(pltpu.with_memory_space_constraint(weight, pltpu.HBM))


def run_experts(own, other, gate_weight, up_weight, down_staged):
    rows, width = own.shape
    hidden = gate_weight.shape[1]
    fast = pl.BlockSpec(memory_space=pltpu.VMEM)
    slow = pl.BlockSpec(memory_space=pl.ANY)
    return pl.pallas_call(
        experts_kernel,
        in_specs=[fast, fast, slow, slow, fast],
        out_specs=[fast] * 2,
        out_shape=[
            jax.ShapeDtypeStruct((rows, width), jnp.float32),
            jax.ShapeDtypeStruct((rows, width), jnp.bfloat16),
        ],
        scratch_shapes=[
            pltpu.VMEM((2 * rows, width), jnp.bfloat16),
            pltpu.VMEM(gate_weight.shape, jnp.bfloat16),
            pltpu.VMEM(up_weight.shape, jnp.bfloat16),
            pltpu.VMEM((2 * rows, hidden), jnp.bfloat16),
            pltpu.SemaphoreType.DMA((2, hidden // min(512, hidden))),
        ],
        compiler_params=pltpu.CompilerParams(vmem_limit_bytes=40 << 20),
        name="experts",
    )(
        own,
        other,
        pltpu.with_memory_space_constraint(gate_weight, pltpu.HBM),
        pltpu.with_memory_space_constraint(up_weight, pltpu.HBM),
        pltpu.with_memory_space_constraint(down_staged, pltpu.VMEM),
    )


def pick(stack, index):
    return lax.dynamic_index_in_dim(stack, index, 0, keepdims=False)


def local(
    hidden_in,
    queries,
    key_new,
    value_new,
    cache_keys,
    cache_values,
    lengths,
    out_weight,
    norm_gain,
    router_weight,
    gate_weight,
    up_weight,
    down_weight,
    routes,
):
    rows, width = hidden_in.shape
    toks = lax.axis_size("tok")
    sides = lax.axis_size("side")
    experts = router_weight.shape[1]
    lines = toks // 2
    half = rows // sides
    cols = out_weight.shape[1]
    span = out_weight.shape[0]
    tok = lax.axis_index("tok")
    side = lax.axis_index("side")
    first_swap = [(t, t ^ 1) for t in range(toks)]
    side_swap = [(0, 1), (1, 0)]

    def across(value):
        return lax.ppermute(value, "side", side_swap)

    def near(value):
        return lax.ppermute(value, "tok", first_swap)

    def line(value, k):
        return lax.ppermute(value, "tok", [(t, t ^ (2 * k)) for t in range(toks)])

    hidden_half = lax.dynamic_slice_in_dim(hidden_in, side * half, half, 0)

    def piece(target):
        part = lax.dynamic_slice_in_dim(hidden_half, target * cols, cols, 1)
        return jnp.concatenate([part[: half // 2], part[half // 2 :]], axis=1)

    attn_out = attend(queries, key_new, value_new, cache_keys, cache_values, lengths)
    down_staged = stage(down_weight)
    arrived = []
    for k in range(lines):
        extra = jnp.concatenate([piece(tok ^ (2 * k)), piece(tok ^ (2 * k) ^ 1)], axis=1)
        extra = extra.reshape(half * 2 * cols // span, span)
        message = jnp.concatenate([attn_out, extra], axis=0)
        arrived.append(line(message, k) if k else message)
    mine = [m[:rows] for m in arrived]
    folded = [m[rows:].reshape(half // 2, 4 * cols) for m in arrived]
    keep = [f[:, : 2 * cols] for f in folded]
    forward = jnp.concatenate([f[:, 2 * cols :] for f in folded], axis=0)
    forward = forward.reshape(lines * half * cols // span, span)
    passed = near(jnp.concatenate(mine + [forward], axis=0))
    theirs = [passed[k * rows : (k + 1) * rows] for k in range(lines)]
    given = passed[lines * rows :].reshape(lines, half // 2, 2 * cols)
    blocks, hidden_blocks = [], []
    for k in range(lines):
        blocks += [mine[k], theirs[k]]
        for f in (keep[k], given[k]):
            hidden_blocks.append(jnp.concatenate([f[:, :cols], f[:, cols:]], axis=0))
    columns = jnp.dot(
        jnp.concatenate(blocks, axis=0), out_weight, preferred_element_type=jnp.float32
    ).reshape(toks, sides, half, cols)
    other = lax.dynamic_index_in_dim(columns, 1 - side, 1, keepdims=False)
    own = lax.dynamic_index_in_dim(columns, side, 1, keepdims=False)
    relative = (
        jnp.stack(hidden_blocks).astype(jnp.float32) + (own + across(other))
    ).astype(jnp.bfloat16)
    residual = jnp.concatenate([pick(relative, tok ^ b) for b in range(toks)], axis=0)
    parts = [residual] + [line(residual, k) for k in range(1, lines)]
    stacked = jnp.stack(parts)
    crossed = near(stacked)
    pieces = jnp.stack([stacked, crossed], axis=1).reshape(toks, toks * half, cols)
    stream = jnp.concatenate([pick(pieces, tok ^ b) for b in range(toks)], axis=1)
    wide = stream.astype(jnp.float32)
    normed = (
        wide * lax.rsqrt(jnp.mean(wide * wide, axis=-1, keepdims=True) + 1e-05) * norm_gain
    ).astype(jnp.bfloat16)
    partner = across(normed)
    own_routes = lax.dynamic_index_in_dim(
        routes.reshape(toks, sides, half, -1), side, 1, keepdims=False
    ).reshape(toks * half, -1)
    coefficient = coefficients(normed, own_routes, router_weight)
    expert = tok // (toks // experts)
    scale = lax.dynamic_slice_in_dim(coefficient, expert, 1, 1)
    partner, scale = lax.optimization_barrier((partner, scale))
    kept, sent = run_experts(
        normed, partner, gate_weight, up_weight, down_staged
    )
    joined = (kept + across(sent).astype(jnp.float32)) * scale
    joined = joined.astype(jnp.bfloat16).reshape(lines, 2, half, width)
    y_own = lax.dynamic_index_in_dim(joined, tok % 2, 1, keepdims=False)
    y_other = lax.dynamic_index_in_dim(joined, 1 - tok % 2, 1, keepdims=False)
    pair = y_own.astype(jnp.float32) + near(y_other).astype(jnp.float32)
    level = tok // 2
    pair_low = pair.astype(jnp.bfloat16)
    total = pick(pair, level)
    for k in range(1, lines):
        total = total + line(pick(pair_low, level ^ k), k).astype(jnp.float32)
    mine_stream = lax.dynamic_slice_in_dim(wide, tok * half, half, 0)
    result = (mine_stream + total).astype(jnp.bfloat16)
    mate = across(result)
    low = jnp.where(side == 0, result, mate)
    high = jnp.where(side == 0, mate, result)
    return jnp.concatenate([low, high], axis=0)


def solution(mesh):
    return jax.shard_map(
        local,
        mesh=mesh,
        in_specs=(
            P(("grp", "tok"), None),
            P(("grp", "tok"), "side", None),
            P(("grp", "tok"), "side", None),
            P(("grp", "tok"), "side", None),
            P(("grp", "tok"), "side", None, None),
            P(("grp", "tok"), "side", None, None),
            P(("grp", "tok")),
            P("side", "tok"),
            P(),
            P(),
            P(None, ("tok", "side")),
            P(None, ("tok", "side")),
            P(("tok", "side"), None),
            P("grp", None),
        ),
        out_specs=P(("grp", "tok"), None),
        check_vma=False,
    )
```

```python
import math

import jax
import jax.numpy as jnp
from jax import lax
from jax.experimental import pallas as pl
from jax.experimental.pallas import tpu as pltpu
from jax.sharding import PartitionSpec as P


def attend(queries, key_new, value_new, cache_keys, cache_values, lengths):
    seq_count, head_count, head_width = queries.shape
    kv_count = key_new.shape[1]
    places = cache_keys.shape[2]
    scaling = 1.0 / math.sqrt(head_width)
    grouped = queries.reshape(seq_count, kv_count, head_count // kv_count, head_width)
    scores = (
        jnp.einsum("skgd,skpd->skgp", grouped, cache_keys, preferred_element_type=jnp.float32)
        * scaling
    )
    usable = jnp.arange(places, dtype=jnp.int32)[None, :] < lengths[:, None]
    scores = jnp.where(usable[:, None, None, :], scores, -jnp.inf)
    own_score = (
        jnp.einsum("skgd,skd->skg", grouped, key_new, preferred_element_type=jnp.float32) * scaling
    )
    top_score = jnp.maximum(jnp.max(scores, axis=-1), own_score)
    weights = jnp.exp(scores - top_score[..., None])
    own_weight = jnp.exp(own_score - top_score)
    totals = jnp.sum(weights, axis=-1) + own_weight
    prob_low = (weights / totals[..., None]).astype(jnp.bfloat16)
    own_low = (own_weight / totals).astype(jnp.bfloat16)
    mixture = jnp.einsum(
        "skgp,skpd->skgd", prob_low, cache_values, preferred_element_type=jnp.float32
    )
    mixture = (
        mixture
        + own_low.astype(jnp.float32)[..., None] * value_new.astype(jnp.float32)[:, :, None, :]
    )
    return mixture.astype(jnp.bfloat16).reshape(seq_count, head_count * head_width)


def scales(normed, picks, mine, router_weight):
    logits = jnp.dot(normed.astype(jnp.float32), router_weight, precision=lax.Precision.HIGHEST)
    chosen = jnp.sum(picks * logits[:, None, :], axis=-1)
    leading = jax.nn.sigmoid(chosen[:, 0] - chosen[:, 1])
    return (leading * mine[:, 0] + (1.0 - leading) * mine[:, 1])[:, None]


def cut(array, start, size, axis):
    return lax.dynamic_slice_in_dim(array, start, size, axis, allow_negative_indices=False)


def experts_kernel(own, other, gate, up, down, kept, sent, block, active):
    rows = own.shape[0]
    step = min(512, gate.shape[1])
    block[:rows] = own[...]
    block[rows:] = other[...]
    for c in range(0, gate.shape[1], step):
        gated = jnp.dot(block[...], gate[:, c : c + step], preferred_element_type=jnp.float32)
        upward = jnp.dot(block[...], up[:, c : c + step], preferred_element_type=jnp.float32)
        active[:, c : c + step] = (jax.nn.silu(gated) * upward).astype(jnp.bfloat16)
    for c in range(0, down.shape[1], 512):
        out = jnp.dot(active[...], down[:, c : c + 512], preferred_element_type=jnp.float32)
        kept[:, c : c + 512] = out[:rows]
        sent[:, c : c + 512] = out[rows:].astype(jnp.bfloat16)


def stage(weight):
    def body(source, target):
        pltpu.sync_copy(source, target)

    return pl.pallas_call(
        body,
        in_specs=[pl.BlockSpec(memory_space=pltpu.HBM)],
        out_specs=pl.BlockSpec(memory_space=pltpu.VMEM),
        out_shape=pltpu.VMEM(weight.shape, weight.dtype),
        cost_estimate=pl.CostEstimate(
            flops=weight.size * 600, transcendentals=0, bytes_accessed=2 * weight.size
        ),
        compiler_params=pltpu.CompilerParams(vmem_limit_bytes=1 << 20),
        name="stage",
    )(pltpu.with_memory_space_constraint(weight, pltpu.HBM))


def run_experts(own, other, *weights):
    rows, width = own.shape
    size = weights[0].size
    fast = pl.BlockSpec(memory_space=pltpu.VMEM)
    return pl.pallas_call(
        experts_kernel,
        in_specs=[fast] * 5,
        out_specs=[fast] * 2,
        out_shape=[
            jax.ShapeDtypeStruct((rows, width), jnp.float32),
            jax.ShapeDtypeStruct((rows, width), jnp.bfloat16),
        ],
        scratch_shapes=[
            pltpu.VMEM((2 * rows, width), jnp.bfloat16),
            pltpu.VMEM((2 * rows, weights[0].shape[1]), jnp.bfloat16),
        ],
        cost_estimate=pl.CostEstimate(
            flops=3 * size * 600, transcendentals=0, bytes_accessed=4 * size
        ),
        compiler_params=pltpu.CompilerParams(vmem_limit_bytes=12 << 20),
        name="experts",
    )(own, other, *[pltpu.with_memory_space_constraint(w, pltpu.VMEM) for w in weights])


def pick(stack, index):
    return cut(stack, index, 1, 0).reshape(stack.shape[1:])


def local(
    hidden_in,
    queries,
    key_new,
    value_new,
    cache_keys,
    cache_values,
    lengths,
    out_weight,
    norm_gain,
    router_weight,
    gate_weight,
    up_weight,
    down_weight,
    routes,
):
    rows, width = hidden_in.shape
    toks = lax.axis_size("tok")
    sides = lax.axis_size("side")
    experts = router_weight.shape[1]
    lines = toks // 2
    half = rows // sides
    cols = out_weight.shape[1]
    span = out_weight.shape[0]
    tok = lax.axis_index("tok")
    side = lax.axis_index("side")
    first_swap = [(t, t ^ 1) for t in range(toks)]
    side_swap = [(0, 1), (1, 0)]

    def across(value):
        return lax.ppermute(value, "side", side_swap)

    def near(value):
        return lax.ppermute(value, "tok", first_swap)

    def line(value, k):
        return lax.ppermute(value, "tok", [(t, t ^ (2 * k)) for t in range(toks)])

    groups = lax.axis_size("grp")
    group = lax.axis_index("grp")
    level = tok // 2
    parity = tok % 2

    def over(value, k):
        return lax.ppermute(value, "grp", [(g, g ^ k) for g in range(groups)])

    shares = groups + 1 if span % (8 * (groups + 1)) == 0 else groups
    share = span // shares
    brought = near(cut(out_weight, group * share, share, 0))
    rest = [near(out_weight[groups * share :])] if shares > groups else []
    gathered = jnp.stack([brought] + [over(brought, k) for k in range(1, groups)])

    hidden_half = cut(hidden_in, side * half, half, 0)
    attn_out = attend(queries, key_new, value_new, cache_keys, cache_values, lengths)
    own_routes = lax.dynamic_slice(
        routes.reshape(lines, 2, sides, half, -1),
        (0, parity, side, 0, 0),
        (lines, 1, 1, half, routes.shape[1]),
        allow_negative_indices=False,
    ).reshape(lines * half, -1)
    expert = tok // (toks // experts)
    picks = (
        own_routes[:, :, None] == jnp.arange(experts, dtype=jnp.int32)[None, None, :]
    ).astype(jnp.float32)
    mine = (own_routes == expert).astype(jnp.float32)
    order = [level ^ b for b in range(lines)]
    starts = [b * (2 * cols) for b in order]
    shares_order = [group ^ b for b in range(groups)]
    even = parity == 0
    first_side = side == 0
    corner = level * half
    (attn_out, picks, mine, order, starts, shares_order, even, first_side, corner, side, away) = (
        lax.optimization_barrier(
            (
                attn_out,
                picks,
                mine,
                order,
                starts,
                shares_order,
                even,
                first_side,
                corner,
                side,
                1 - side,
            )
        )
    )
    staged = [stage(w) for w in (gate_weight, up_weight, down_weight)]
    arrived = []
    for k in range(lines):
        part = cut(hidden_half, starts[k], 2 * cols, 1)
        folds = span // (2 * cols)
        deep = half // folds
        extra = jnp.concatenate([part[i * deep : (i + 1) * deep] for i in range(folds)], axis=1)
        message = jnp.concatenate([attn_out, extra], axis=0)
        arrived.append(line(message, k) if k else message)
    arrived, staged[0] = lax.optimization_barrier((arrived, staged[0]))
    blocks = jnp.concatenate([m[:rows] for m in arrived], axis=0)
    hidden_blocks = jnp.stack(
        [
            jnp.concatenate(
                [m[rows:, i * 2 * cols : (i + 1) * 2 * cols] for i in range(folds)], axis=0
            )
            for m in arrived
        ]
    )
    far_weight = jnp.concatenate([pick(gathered, b) for b in shares_order] + rest, axis=0)
    own_columns = jnp.dot(blocks, out_weight, preferred_element_type=jnp.float32)
    far_columns = jnp.dot(blocks, far_weight, preferred_element_type=jnp.float32)
    columns = jnp.concatenate(
        [
            jnp.where(even, own_columns, far_columns),
            jnp.where(even, far_columns, own_columns),
        ],
        axis=1,
    ).reshape(lines, sides, half, 2 * cols)
    other = cut(columns, away, 1, 1).reshape(lines, half, 2 * cols)
    own = cut(columns, side, 1, 1).reshape(lines, half, 2 * cols)
    relative = (hidden_blocks.astype(jnp.float32) + (own + across(other))).astype(jnp.bfloat16)
    residual = jnp.concatenate([pick(relative, b) for b in order], axis=0)
    parts = jnp.stack([residual] + [line(residual, k) for k in range(1, lines)])
    parts, staged = lax.optimization_barrier((parts, staged))
    stream = jnp.concatenate([pick(parts, b) for b in order], axis=1)
    wide = stream.astype(jnp.float32)
    normed = (
        wide * lax.rsqrt(jnp.mean(wide * wide, axis=-1, keepdims=True) + 1e-05) * norm_gain
    ).astype(jnp.bfloat16)
    distant = near(normed)
    mate_rows = across(normed)
    scale = scales(normed, picks, mine, router_weight)
    kept, sent = run_experts(normed, mate_rows, *staged)
    distant, sent = lax.optimization_barrier((distant, sent))
    back = across(sent)
    far_mates = across(distant)
    far_mates, back = lax.optimization_barrier((far_mates, back))
    far_kept, far_sent = run_experts(distant, far_mates, *staged)
    outward = (far_kept + across(far_sent).astype(jnp.float32)).astype(jnp.bfloat16)
    local_sum = kept + back.astype(jnp.float32)
    pair = ((local_sum + near(outward).astype(jnp.float32)) * scale).reshape(lines, half, width)
    pair_low = pair.astype(jnp.bfloat16)
    total = pick(pair, order[0])
    for k in range(1, lines):
        total = total + line(pick(pair_low, order[k]), k).astype(jnp.float32)
    mine_stream = cut(wide, corner, half, 0)
    result = (mine_stream + total).astype(jnp.bfloat16)
    mate = across(result)
    low = jnp.where(first_side, result, mate)
    high = jnp.where(first_side, mate, result)
    return jnp.concatenate([low, high], axis=0)


def solution(mesh):
    return jax.shard_map(
        local,
        mesh=mesh,
        in_specs=(
            P(("grp", "tok"), None),
            P(("grp", "tok"), "side", None),
            P(("grp", "tok"), "side", None),
            P(("grp", "tok"), "side", None),
            P(("grp", "tok"), "side", None, None),
            P(("grp", "tok"), "side", None, None),
            P(("grp", "tok")),
            P("side", "tok"),
            P(),
            P(),
            P(None, ("tok", "side")),
            P(None, ("tok", "side")),
            P(("tok", "side"), None),
            P("grp", None),
        ),
        out_specs=P(("grp", "tok"), None),
        check_vma=False,
    )
```

```python
import math

import jax
import jax.numpy as jnp
from jax import lax
from jax.experimental import pallas as pl
from jax.experimental.pallas import tpu as pltpu
from jax.sharding import PartitionSpec as P


def attend(queries, key_new, value_new, cache_keys, cache_values, lengths):
    seq_count, head_count, head_width = queries.shape
    kv_count = key_new.shape[1]
    places = cache_keys.shape[2]
    scaling = 1.0 / math.sqrt(head_width)
    grouped = queries.reshape(seq_count, kv_count, head_count // kv_count, head_width)
    scores = (
        jnp.einsum("skgd,skpd->skgp", grouped, cache_keys, preferred_element_type=jnp.float32)
        * scaling
    )
    usable = jnp.arange(places, dtype=jnp.int32)[None, :] < lengths[:, None]
    scores = jnp.where(usable[:, None, None, :], scores, -jnp.inf)
    own_score = (
        jnp.einsum("skgd,skd->skg", grouped, key_new, preferred_element_type=jnp.float32) * scaling
    )
    top_score = jnp.maximum(jnp.max(scores, axis=-1), own_score)
    weights = jnp.exp(scores - top_score[..., None])
    own_weight = jnp.exp(own_score - top_score)
    totals = jnp.sum(weights, axis=-1) + own_weight
    prob_low = (weights / totals[..., None]).astype(jnp.bfloat16)
    own_low = (own_weight / totals).astype(jnp.bfloat16)
    mixture = jnp.einsum(
        "skgp,skpd->skgd", prob_low, cache_values, preferred_element_type=jnp.float32
    )
    mixture = (
        mixture
        + own_low.astype(jnp.float32)[..., None] * value_new.astype(jnp.float32)[:, :, None, :]
    )
    return mixture.astype(jnp.bfloat16).reshape(seq_count, head_count * head_width)


def scales(normed, picks, mine, router_weight):
    logits = jnp.dot(normed.astype(jnp.float32), router_weight, precision=lax.Precision.HIGHEST)
    chosen = jnp.sum(picks * logits[:, None, :], axis=-1)
    leading = jax.nn.sigmoid(chosen[:, 0] - chosen[:, 1])
    return (leading * mine[:, 0] + (1.0 - leading) * mine[:, 1])[:, None]


def cut(array, start, size, axis):
    return lax.dynamic_slice_in_dim(array, start, size, axis, allow_negative_indices=False)


def experts_kernel(own, other, gate, up, down, kept, sent, block, active):
    rows = own.shape[0]
    step = min(512, gate.shape[1])
    block[:rows] = own[...]
    block[rows:] = other[...]
    for c in range(0, gate.shape[1], step):
        gated = jnp.dot(block[...], gate[:, c : c + step], preferred_element_type=jnp.float32)
        upward = jnp.dot(block[...], up[:, c : c + step], preferred_element_type=jnp.float32)
        active[:, c : c + step] = (jax.nn.silu(gated) * upward).astype(jnp.bfloat16)
    for c in range(0, down.shape[1], 512):
        out = jnp.dot(active[...], down[:, c : c + 512], preferred_element_type=jnp.float32)
        kept[:, c : c + 512] = out[:rows]
        sent[:, c : c + 512] = out[rows:].astype(jnp.bfloat16)


def stage(weight):
    def body(source, target):
        pltpu.sync_copy(source, target)

    return pl.pallas_call(
        body,
        in_specs=[pl.BlockSpec(memory_space=pltpu.HBM)],
        out_specs=pl.BlockSpec(memory_space=pltpu.VMEM),
        out_shape=pltpu.VMEM(weight.shape, weight.dtype),
        cost_estimate=pl.CostEstimate(
            flops=weight.size * 600, transcendentals=0, bytes_accessed=2 * weight.size
        ),
        compiler_params=pltpu.CompilerParams(vmem_limit_bytes=1 << 20),
        name="stage",
    )(pltpu.with_memory_space_constraint(weight, pltpu.HBM))


def run_experts(own, other, *weights):
    rows, width = own.shape
    size = weights[0].size
    fast = pl.BlockSpec(memory_space=pltpu.VMEM)
    return pl.pallas_call(
        experts_kernel,
        in_specs=[fast] * 5,
        out_specs=[fast] * 2,
        out_shape=[
            jax.ShapeDtypeStruct((rows, width), jnp.float32),
            jax.ShapeDtypeStruct((rows, width), jnp.bfloat16),
        ],
        scratch_shapes=[
            pltpu.VMEM((2 * rows, width), jnp.bfloat16),
            pltpu.VMEM((2 * rows, weights[0].shape[1]), jnp.bfloat16),
        ],
        cost_estimate=pl.CostEstimate(
            flops=3 * size * 600, transcendentals=0, bytes_accessed=4 * size
        ),
        compiler_params=pltpu.CompilerParams(vmem_limit_bytes=12 << 20),
        name="experts",
    )(own, other, *[pltpu.with_memory_space_constraint(w, pltpu.VMEM) for w in weights])


def pick(stack, index):
    return cut(stack, index, 1, 0).reshape(stack.shape[1:])


def local(
    hidden_in,
    queries,
    key_new,
    value_new,
    cache_keys,
    cache_values,
    lengths,
    out_weight,
    norm_gain,
    router_weight,
    gate_weight,
    up_weight,
    down_weight,
    routes,
):
    rows, width = hidden_in.shape
    toks = lax.axis_size("tok")
    sides = lax.axis_size("side")
    experts = router_weight.shape[1]
    lines = toks // 2
    half = rows // sides
    cols = out_weight.shape[1]
    span = out_weight.shape[0]
    tok = lax.axis_index("tok")
    side = lax.axis_index("side")
    first_swap = [(t, t ^ 1) for t in range(toks)]
    side_swap = [(0, 1), (1, 0)]

    def across(value):
        return lax.ppermute(value, "side", side_swap)

    def near(value):
        return lax.ppermute(value, "tok", first_swap)

    def line(value, k):
        return lax.ppermute(value, "tok", [(t, t ^ (2 * k)) for t in range(toks)])

    groups = lax.axis_size("grp")
    group = lax.axis_index("grp")
    level = tok // 2
    parity = tok % 2

    def over(value, k):
        return lax.ppermute(value, "grp", [(g, g ^ k) for g in range(groups)])

    shares = groups + 1 if span % (8 * (groups + 1)) == 0 else groups
    share = span // shares
    brought = near(cut(out_weight, group * share, share, 0))
    rest = [near(out_weight[groups * share :])] if shares > groups else []
    gathered = jnp.stack([brought] + [over(brought, k) for k in range(1, groups)])

    hidden_half = cut(hidden_in, side * half, half, 0)
    attn_out = attend(queries, key_new, value_new, cache_keys, cache_values, lengths)
    expert = tok // (toks // experts)
    expert_ids = jnp.arange(experts, dtype=jnp.int32)

    def masks(which):
        chosen = lax.dynamic_slice(
            routes.reshape(lines, 2, sides, half, -1),
            (0, which, side, 0, 0),
            (lines, 1, 1, half, routes.shape[1]),
            allow_negative_indices=False,
        ).reshape(lines * half, -1)
        picks = (chosen[:, :, None] == expert_ids[None, None, :]).astype(jnp.float32)
        return picks, (chosen == expert).astype(jnp.float32)

    own_masks, far_masks = masks(parity), masks(1 - parity)
    order = [level ^ b for b in range(lines)]
    starts = [b * (2 * cols) for b in order]
    shares_order = [group ^ b for b in range(groups)]
    even = parity == 0
    first_side = side == 0
    corner = level * half
    (attn_out, own_masks, far_masks, order, starts, shares_order, even, first_side, corner, side, away) = (
        lax.optimization_barrier(
            (
                attn_out,
                own_masks,
                far_masks,
                order,
                starts,
                shares_order,
                even,
                first_side,
                corner,
                side,
                1 - side,
            )
        )
    )
    staged = [stage(w) for w in (gate_weight, up_weight, down_weight)]
    arrived = []
    for k in range(lines):
        part = cut(hidden_half, starts[k], 2 * cols, 1)
        folds = span // (2 * cols)
        deep = half // folds
        extra = jnp.concatenate([part[i * deep : (i + 1) * deep] for i in range(folds)], axis=1)
        message = jnp.concatenate([attn_out, extra], axis=0)
        arrived.append(line(message, k) if k else message)
    arrived, staged[0] = lax.optimization_barrier((arrived, staged[0]))
    blocks = jnp.concatenate([m[:rows] for m in arrived], axis=0)
    hidden_blocks = jnp.stack(
        [
            jnp.concatenate(
                [m[rows:, i * 2 * cols : (i + 1) * 2 * cols] for i in range(folds)], axis=0
            )
            for m in arrived
        ]
    )
    far_weight = jnp.concatenate([pick(gathered, b) for b in shares_order] + rest, axis=0)
    own_columns = jnp.dot(blocks, out_weight, preferred_element_type=jnp.float32)
    far_columns = jnp.dot(blocks, far_weight, preferred_element_type=jnp.float32)
    columns = jnp.concatenate(
        [
            jnp.where(even, own_columns, far_columns),
            jnp.where(even, far_columns, own_columns),
        ],
        axis=1,
    ).reshape(lines, sides, half, 2 * cols)
    other = cut(columns, away, 1, 1).reshape(lines, half, 2 * cols)
    own = cut(columns, side, 1, 1).reshape(lines, half, 2 * cols)
    relative = (hidden_blocks.astype(jnp.float32) + (own + across(other))).astype(jnp.bfloat16)
    residual = jnp.concatenate([pick(relative, b) for b in order], axis=0)
    parts = jnp.stack([residual] + [line(residual, k) for k in range(1, lines)])
    parts, staged = lax.optimization_barrier((parts, staged))
    stream = jnp.concatenate([pick(parts, b) for b in order], axis=1)
    wide = stream.astype(jnp.float32)
    normed = (
        wide * lax.rsqrt(jnp.mean(wide * wide, axis=-1, keepdims=True) + 1e-05) * norm_gain
    ).astype(jnp.bfloat16)
    distant = near(normed)
    mate_rows = across(normed)
    mine_stream = lax.optimization_barrier(cut(wide, corner, half, 0) * 1.0)
    scale = scales(normed, *own_masks, router_weight)
    kept, sent = run_experts(normed, mate_rows, *staged)
    back = across(sent)

    def reduce_line(values, weights):
        weighted = (values * weights).reshape(lines, half, width)
        low = weighted.astype(jnp.bfloat16)
        return pick(weighted, order[0]), [
            line(pick(low, order[k]), k) for k in range(1, lines)
        ]

    own_part, own_others = reduce_line(kept + back.astype(jnp.float32), scale)
    distant, _ = lax.optimization_barrier((distant, own_part))
    far_mates = across(distant)
    far_kept, far_sent = run_experts(distant, far_mates, *staged)
    far_scale = scales(distant, *far_masks, router_weight)
    far_part, far_others = reduce_line(
        far_kept + across(far_sent).astype(jnp.float32), far_scale
    )
    for value in far_others:
        far_part = far_part + value.astype(jnp.float32)
    total = own_part
    for value in own_others + [near(far_part.astype(jnp.bfloat16))]:
        total = total + value.astype(jnp.float32)
    result = (mine_stream + total).astype(jnp.bfloat16)
    mate = across(result)
    low = jnp.where(first_side, result, mate)
    high = jnp.where(first_side, mate, result)
    return jnp.concatenate([low, high], axis=0)


def solution(mesh):
    return jax.shard_map(
        local,
        mesh=mesh,
        in_specs=(
            P(("grp", "tok"), None),
            P(("grp", "tok"), "side", None),
            P(("grp", "tok"), "side", None),
            P(("grp", "tok"), "side", None),
            P(("grp", "tok"), "side", None, None),
            P(("grp", "tok"), "side", None, None),
            P(("grp", "tok")),
            P("side", "tok"),
            P(),
            P(),
            P(None, ("tok", "side")),
            P(None, ("tok", "side")),
            P(("tok", "side"), None),
            P("grp", None),
        ),
        out_specs=P(("grp", "tok"), None),
        check_vma=False,
    )
```

```python
import math

import jax
import jax.numpy as jnp
from jax import lax
from jax.experimental import pallas as pl
from jax.experimental.pallas import tpu as pltpu
from jax.sharding import PartitionSpec as P


def attend(queries, key_new, value_new, cache_keys, cache_values, lengths):
    seq_count, head_count, head_width = queries.shape
    kv_count = key_new.shape[1]
    places = cache_keys.shape[2]
    scaling = 1.0 / math.sqrt(head_width)
    grouped = queries.reshape(seq_count, kv_count, head_count // kv_count, head_width)
    scores = (
        jnp.einsum("skgd,skpd->skgp", grouped, cache_keys, preferred_element_type=jnp.float32)
        * scaling
    )
    usable = jnp.arange(places, dtype=jnp.int32)[None, :] < lengths[:, None]
    scores = jnp.where(usable[:, None, None, :], scores, -jnp.inf)
    own_score = (
        jnp.einsum("skgd,skd->skg", grouped, key_new, preferred_element_type=jnp.float32) * scaling
    )
    top_score = jnp.maximum(jnp.max(scores, axis=-1), own_score)
    weights = jnp.exp(scores - top_score[..., None])
    own_weight = jnp.exp(own_score - top_score)
    totals = jnp.sum(weights, axis=-1) + own_weight
    prob_low = (weights / totals[..., None]).astype(jnp.bfloat16)
    own_low = (own_weight / totals).astype(jnp.bfloat16)
    mixture = jnp.einsum(
        "skgp,skpd->skgd", prob_low, cache_values, preferred_element_type=jnp.float32
    )
    mixture = (
        mixture
        + own_low.astype(jnp.float32)[..., None] * value_new.astype(jnp.float32)[:, :, None, :]
    )
    return mixture.astype(jnp.bfloat16).reshape(seq_count, head_count * head_width)


def scales(normed, picks, mine, router_weight):
    logits = jnp.dot(normed.astype(jnp.float32), router_weight, precision=lax.Precision.HIGHEST)
    chosen = jnp.sum(picks * logits[:, None, :], axis=-1)
    leading = jax.nn.sigmoid(chosen[:, 0] - chosen[:, 1])
    return (leading * mine[:, 0] + (1.0 - leading) * mine[:, 1])[:, None]


def cut(array, start, size, axis):
    return lax.dynamic_slice_in_dim(array, start, size, axis, allow_negative_indices=False)


def experts_kernel(own, other, gate, up, down, kept, sent, block, active):
    rows = own.shape[0]
    step = min(512, gate.shape[1])
    block[:rows] = own[...]
    block[rows:] = other[...]
    for c in range(0, gate.shape[1], step):
        gated = jnp.dot(block[...], gate[:, c : c + step], preferred_element_type=jnp.float32)
        upward = jnp.dot(block[...], up[:, c : c + step], preferred_element_type=jnp.float32)
        active[:, c : c + step] = (jax.nn.silu(gated) * upward).astype(jnp.bfloat16)
    for c in range(0, down.shape[1], 512):
        out = jnp.dot(active[...], down[:, c : c + 512], preferred_element_type=jnp.float32)
        kept[:, c : c + 512] = out[:rows]
        sent[:, c : c + 512] = out[rows:].astype(jnp.bfloat16)


def stage(weight):
    def body(source, target):
        pltpu.sync_copy(source, target)

    return pl.pallas_call(
        body,
        in_specs=[pl.BlockSpec(memory_space=pltpu.HBM)],
        out_specs=pl.BlockSpec(memory_space=pltpu.VMEM),
        out_shape=pltpu.VMEM(weight.shape, weight.dtype),
        cost_estimate=pl.CostEstimate(
            flops=weight.size * 600, transcendentals=0, bytes_accessed=2 * weight.size
        ),
        compiler_params=pltpu.CompilerParams(vmem_limit_bytes=1 << 20),
        name="stage",
    )(pltpu.with_memory_space_constraint(weight, pltpu.HBM))


def run_experts(own, other, *weights):
    rows, width = own.shape
    size = weights[0].size
    fast = pl.BlockSpec(memory_space=pltpu.VMEM)
    return pl.pallas_call(
        experts_kernel,
        in_specs=[fast] * 5,
        out_specs=[fast] * 2,
        out_shape=[
            jax.ShapeDtypeStruct((rows, width), jnp.float32),
            jax.ShapeDtypeStruct((rows, width), jnp.bfloat16),
        ],
        scratch_shapes=[
            pltpu.VMEM((2 * rows, width), jnp.bfloat16),
            pltpu.VMEM((2 * rows, weights[0].shape[1]), jnp.bfloat16),
        ],
        cost_estimate=pl.CostEstimate(
            flops=3 * size * 600, transcendentals=0, bytes_accessed=4 * size
        ),
        compiler_params=pltpu.CompilerParams(vmem_limit_bytes=12 << 20),
        name="experts",
    )(own, other, *[pltpu.with_memory_space_constraint(w, pltpu.VMEM) for w in weights])


def pick(stack, index):
    return cut(stack, index, 1, 0).reshape(stack.shape[1:])


def local(
    hidden_in,
    queries,
    key_new,
    value_new,
    cache_keys,
    cache_values,
    lengths,
    out_weight,
    norm_gain,
    router_weight,
    gate_weight,
    up_weight,
    down_weight,
    routes,
):
    rows, width = hidden_in.shape
    toks = lax.axis_size("tok")
    sides = lax.axis_size("side")
    experts = router_weight.shape[1]
    lines = toks // 2
    half = rows // sides
    cols = out_weight.shape[1]
    span = out_weight.shape[0]
    tok = lax.axis_index("tok")
    side = lax.axis_index("side")
    first_swap = [(t, t ^ 1) for t in range(toks)]
    side_swap = [(0, 1), (1, 0)]

    def across(value):
        return lax.ppermute(value, "side", side_swap)

    def near(value):
        return lax.ppermute(value, "tok", first_swap)

    def line(value, k):
        return lax.ppermute(value, "tok", [(t, t ^ (2 * k)) for t in range(toks)])

    groups = lax.axis_size("grp")
    group = lax.axis_index("grp")
    level = tok // 2
    parity = tok % 2

    def over(value, k):
        return lax.ppermute(value, "grp", [(g, g ^ k) for g in range(groups)])

    shares = groups + 1 if span % (8 * (groups + 1)) == 0 else groups
    share = span // shares
    brought = near(cut(out_weight, group * share, share, 0))
    rest = [near(out_weight[groups * share :])] if shares > groups else []
    gathered = jnp.stack([brought] + [over(brought, k) for k in range(1, groups)])

    hidden_half = cut(hidden_in, side * half, half, 0)
    expert = tok // (toks // experts)
    expert_ids = jnp.arange(experts, dtype=jnp.int32)

    def masks(which):
        chosen = lax.dynamic_slice(
            routes.reshape(lines, 2, sides, half, -1),
            (0, which, side, 0, 0),
            (lines, 1, 1, half, routes.shape[1]),
            allow_negative_indices=False,
        ).reshape(lines * half, -1)
        picks = (chosen[:, :, None] == expert_ids[None, None, :]).astype(jnp.float32)
        return picks, (chosen == expert).astype(jnp.float32)

    own_masks, far_masks = masks(parity), masks(1 - parity)
    order = [level ^ b for b in range(lines)]
    starts = [b * (2 * cols) for b in order]
    shares_order = [group ^ b for b in range(groups)]
    even = parity == 0
    first_side = side == 0
    corner = level * half
    ahead = (own_masks, far_masks, order, starts, shares_order, even, first_side, corner, side)
    queries, ahead, away = lax.optimization_barrier((queries, ahead, 1 - side))
    own_masks, far_masks, order, starts, shares_order, even, first_side, corner, side = ahead
    attn_out = attend(queries, key_new, value_new, cache_keys, cache_values, lengths)
    staged = [stage(w) for w in (gate_weight, up_weight, down_weight)]
    arrived = []
    for k in range(lines):
        part = cut(hidden_half, starts[k], 2 * cols, 1)
        folds = span // (2 * cols)
        deep = half // folds
        extra = jnp.concatenate([part[i * deep : (i + 1) * deep] for i in range(folds)], axis=1)
        message = jnp.concatenate([attn_out, extra], axis=0)
        arrived.append(line(message, k) if k else message)
    arrived, staged[0] = lax.optimization_barrier((arrived, staged[0]))
    blocks = jnp.concatenate([m[:rows] for m in arrived], axis=0)
    hidden_blocks = jnp.stack(
        [
            jnp.concatenate(
                [m[rows:, i * 2 * cols : (i + 1) * 2 * cols] for i in range(folds)], axis=0
            )
            for m in arrived
        ]
    )
    far_weight = jnp.concatenate([pick(gathered, b) for b in shares_order] + rest, axis=0)
    own_columns = jnp.dot(blocks, out_weight, preferred_element_type=jnp.float32)
    far_columns = jnp.dot(blocks, far_weight, preferred_element_type=jnp.float32)
    columns = jnp.concatenate(
        [
            jnp.where(even, own_columns, far_columns),
            jnp.where(even, far_columns, own_columns),
        ],
        axis=1,
    ).reshape(lines, sides, half, 2 * cols)
    other = cut(columns, away, 1, 1).reshape(lines, half, 2 * cols)
    own = cut(columns, side, 1, 1).reshape(lines, half, 2 * cols)
    relative = (hidden_blocks.astype(jnp.float32) + (own + across(other))).astype(jnp.bfloat16)
    residual = jnp.concatenate([pick(relative, b) for b in order], axis=0)
    parts = jnp.stack([residual] + [line(residual, k) for k in range(1, lines)])
    parts, staged = lax.optimization_barrier((parts, staged))
    stream = jnp.concatenate([pick(parts, b) for b in order], axis=1)
    wide = stream.astype(jnp.float32)
    normed = (
        wide * lax.rsqrt(jnp.mean(wide * wide, axis=-1, keepdims=True) + 1e-05) * norm_gain
    ).astype(jnp.bfloat16)
    distant = near(normed)
    mate_rows = across(normed)
    mine_stream = lax.optimization_barrier(cut(wide, corner, half, 0) * 1.0)
    scale = scales(normed, *own_masks, router_weight)
    kept, sent = run_experts(normed, mate_rows, *staged)
    back = across(sent)

    def reduce_line(values, weights):
        weighted = (values * weights).reshape(lines, half, width)
        low = weighted.astype(jnp.bfloat16)
        others = []
        for k in range(1, lines):
            others.append(line(pick(low, order[k]), k))
        return pick(weighted, order[0]), others

    own_part, own_others = reduce_line(kept + back.astype(jnp.float32), scale)
    distant, _ = lax.optimization_barrier((distant, own_part))
    far_mates = across(distant)
    far_kept, far_sent = run_experts(distant, far_mates, *staged)
    far_scale = scales(distant, *far_masks, router_weight)
    far_part, far_others = reduce_line(
        far_kept + across(far_sent).astype(jnp.float32), far_scale
    )
    for value in far_others:
        far_part = far_part + value.astype(jnp.float32)
    total = own_part
    for value in own_others + [near(far_part.astype(jnp.bfloat16))]:
        total = total + value.astype(jnp.float32)
    result = (mine_stream + total).astype(jnp.bfloat16)
    mate = across(result)
    low = jnp.where(first_side, result, mate)
    high = jnp.where(first_side, mate, result)
    return jnp.concatenate([low, high], axis=0)


def solution(mesh):
    return jax.shard_map(
        local,
        mesh=mesh,
        in_specs=(
            P(("grp", "tok"), None),
            P(("grp", "tok"), "side", None),
            P(("grp", "tok"), "side", None),
            P(("grp", "tok"), "side", None),
            P(("grp", "tok"), "side", None, None),
            P(("grp", "tok"), "side", None, None),
            P(("grp", "tok")),
            P("side", "tok"),
            P(),
            P(),
            P(None, ("tok", "side")),
            P(None, ("tok", "side")),
            P(("tok", "side"), None),
            P("grp", None),
        ),
        out_specs=P(("grp", "tok"), None),
        check_vma=False,
    )
```

```python
import math

import jax
import jax.numpy as jnp
from jax import lax
from jax.experimental import pallas as pl
from jax.experimental.pallas import tpu as pltpu
from jax.sharding import PartitionSpec as P


def attend(queries, key_new, value_new, cache_keys, cache_values, lengths):
    seq_count, head_count, head_width = queries.shape
    kv_count = key_new.shape[1]
    places = cache_keys.shape[2]
    scaling = 1.0 / math.sqrt(head_width)
    grouped = queries.reshape(seq_count, kv_count, head_count // kv_count, head_width)
    scores = (
        jnp.einsum("skgd,skpd->skgp", grouped, cache_keys, preferred_element_type=jnp.float32)
        * scaling
    )
    usable = jnp.arange(places, dtype=jnp.int32)[None, :] < lengths[:, None]
    scores = jnp.where(usable[:, None, None, :], scores, -jnp.inf)
    own_score = (
        jnp.einsum("skgd,skd->skg", grouped, key_new, preferred_element_type=jnp.float32) * scaling
    )
    top_score = jnp.maximum(jnp.max(scores, axis=-1), own_score)
    weights = jnp.exp(scores - top_score[..., None])
    own_weight = jnp.exp(own_score - top_score)
    totals = jnp.sum(weights, axis=-1) + own_weight
    prob_low = (weights / totals[..., None]).astype(jnp.bfloat16)
    own_low = (own_weight / totals).astype(jnp.bfloat16)
    mixture = jnp.einsum(
        "skgp,skpd->skgd", prob_low, cache_values, preferred_element_type=jnp.float32
    )
    mixture = (
        mixture
        + own_low.astype(jnp.float32)[..., None] * value_new.astype(jnp.float32)[:, :, None, :]
    )
    return mixture.astype(jnp.bfloat16).reshape(seq_count, head_count * head_width)


def scales(normed, picks, mine, router_weight):
    logits = jnp.dot(normed.astype(jnp.float32), router_weight, precision=lax.Precision.HIGHEST)
    chosen = jnp.sum(picks * logits[:, None, :], axis=-1)
    leading = jax.nn.sigmoid(chosen[:, 0] - chosen[:, 1])
    return (leading * mine[:, 0] + (1.0 - leading) * mine[:, 1])[:, None]


def cut(array, start, size, axis):
    return lax.dynamic_slice_in_dim(array, start, size, axis, allow_negative_indices=False)


def experts_kernel(own, other, gate, up, down, kept, sent, block, active):
    rows = own.shape[0]
    step = min(512, gate.shape[1])
    block[:rows] = own[...]
    block[rows:] = other[...]
    for c in range(0, gate.shape[1], step):
        gated = jnp.dot(block[...], gate[:, c : c + step], preferred_element_type=jnp.float32)
        upward = jnp.dot(block[...], up[:, c : c + step], preferred_element_type=jnp.float32)
        active[:, c : c + step] = (jax.nn.silu(gated) * upward).astype(jnp.bfloat16)
    for c in range(0, down.shape[1], 512):
        out = jnp.dot(active[...], down[:, c : c + 512], preferred_element_type=jnp.float32)
        kept[:, c : c + 512] = out[:rows]
        sent[:, c : c + 512] = out[rows:].astype(jnp.bfloat16)


def stage(weight):
    def body(source, target):
        pltpu.sync_copy(source, target)

    return pl.pallas_call(
        body,
        in_specs=[pl.BlockSpec(memory_space=pltpu.HBM)],
        out_specs=pl.BlockSpec(memory_space=pltpu.VMEM),
        out_shape=pltpu.VMEM(weight.shape, weight.dtype),
        cost_estimate=pl.CostEstimate(
            flops=weight.size * 600, transcendentals=0, bytes_accessed=2 * weight.size
        ),
        compiler_params=pltpu.CompilerParams(vmem_limit_bytes=1 << 20),
        name="stage",
    )(pltpu.with_memory_space_constraint(weight, pltpu.HBM))


def run_experts(own, other, *weights):
    rows, width = own.shape
    size = weights[0].size
    fast = pl.BlockSpec(memory_space=pltpu.VMEM)
    return pl.pallas_call(
        experts_kernel,
        in_specs=[fast] * 5,
        out_specs=[fast] * 2,
        out_shape=[
            jax.ShapeDtypeStruct((rows, width), jnp.float32),
            jax.ShapeDtypeStruct((rows, width), jnp.bfloat16),
        ],
        scratch_shapes=[
            pltpu.VMEM((2 * rows, width), jnp.bfloat16),
            pltpu.VMEM((2 * rows, weights[0].shape[1]), jnp.bfloat16),
        ],
        cost_estimate=pl.CostEstimate(
            flops=3 * size * 600, transcendentals=0, bytes_accessed=4 * size
        ),
        compiler_params=pltpu.CompilerParams(vmem_limit_bytes=12 << 20),
        name="experts",
    )(own, other, *[pltpu.with_memory_space_constraint(w, pltpu.VMEM) for w in weights])


def pick(stack, index):
    return cut(stack, index, 1, 0).reshape(stack.shape[1:])


def local(
    hidden_in,
    queries,
    key_new,
    value_new,
    cache_keys,
    cache_values,
    lengths,
    out_weight,
    norm_gain,
    router_weight,
    gate_weight,
    up_weight,
    down_weight,
    routes,
):
    rows, width = hidden_in.shape
    toks = lax.axis_size("tok")
    sides = lax.axis_size("side")
    experts = router_weight.shape[1]
    lines = toks // 2
    half = rows // sides
    cols = out_weight.shape[1]
    span = out_weight.shape[0]
    tok = lax.axis_index("tok")
    side = lax.axis_index("side")
    first_swap = [(t, t ^ 1) for t in range(toks)]
    side_swap = [(0, 1), (1, 0)]

    def across(value):
        return lax.ppermute(value, "side", side_swap)

    def near(value):
        return lax.ppermute(value, "tok", first_swap)

    def line(value, k):
        return lax.ppermute(value, "tok", [(t, t ^ (2 * k)) for t in range(toks)])

    groups = lax.axis_size("grp")
    group = lax.axis_index("grp")
    level = tok // 2
    parity = tok % 2

    def over(value, k):
        return lax.ppermute(value, "grp", [(g, g ^ k) for g in range(groups)])

    shares = groups + 1 if span % (8 * (groups + 1)) == 0 else groups
    share = span // shares
    brought = near(cut(out_weight, group * share, share, 0))
    rest = [near(out_weight[groups * share :])] if shares > groups else []
    gathered = jnp.stack([brought] + [over(brought, k) for k in range(1, groups)])

    hidden_half = cut(hidden_in, side * half, half, 0)
    expert = tok // (toks // experts)
    expert_ids = jnp.arange(experts, dtype=jnp.int32)

    def masks(which):
        chosen = lax.dynamic_slice(
            routes.reshape(lines, 2, sides, half, -1),
            (0, which, side, 0, 0),
            (lines, 1, 1, half, routes.shape[1]),
            allow_negative_indices=False,
        ).reshape(lines * half, -1)
        picks = (chosen[:, :, None] == expert_ids[None, None, :]).astype(jnp.float32)
        return picks, (chosen == expert).astype(jnp.float32)

    own_masks, far_masks = masks(parity), masks(1 - parity)
    order = [level ^ b for b in range(lines)]
    starts = [b * (2 * cols) for b in order]
    shares_order = [group ^ b for b in range(groups)]
    even = parity == 0
    first_side = side == 0
    corner = level * half
    ahead = (own_masks, far_masks, order, starts, shares_order, even, first_side, corner, side)
    queries, ahead, away = lax.optimization_barrier((queries, ahead, 1 - side))
    own_masks, far_masks, order, starts, shares_order, even, first_side, corner, side = ahead
    attn_out = attend(queries, key_new, value_new, cache_keys, cache_values, lengths)
    up_staged = stage(up_weight)
    staged = [stage(gate_weight), up_staged, stage(down_weight)]
    arrived = []
    for k in range(lines):
        part = cut(hidden_half, starts[k], 2 * cols, 1)
        folds = span // (2 * cols)
        deep = half // folds
        extra = jnp.concatenate([part[i * deep : (i + 1) * deep] for i in range(folds)], axis=1)
        message = jnp.concatenate([attn_out, extra], axis=0)
        arrived.append(line(message, k) if k else message)
    arrived, staged[:2] = lax.optimization_barrier((arrived, staged[:2]))
    blocks = jnp.concatenate([m[:rows] for m in arrived], axis=0)
    hidden_blocks = jnp.stack(
        [
            jnp.concatenate(
                [m[rows:, i * 2 * cols : (i + 1) * 2 * cols] for i in range(folds)], axis=0
            )
            for m in arrived
        ]
    )
    far_weight = jnp.concatenate([pick(gathered, b) for b in shares_order] + rest, axis=0)
    own_columns = jnp.dot(blocks, out_weight, preferred_element_type=jnp.float32)
    far_columns = jnp.dot(blocks, far_weight, preferred_element_type=jnp.float32)
    columns = jnp.concatenate(
        [
            jnp.where(even, own_columns, far_columns),
            jnp.where(even, far_columns, own_columns),
        ],
        axis=1,
    ).reshape(lines, sides, half, 2 * cols)
    other = cut(columns, away, 1, 1).reshape(lines, half, 2 * cols)
    own = cut(columns, side, 1, 1).reshape(lines, half, 2 * cols)
    relative = (hidden_blocks.astype(jnp.float32) + (own + across(other))).astype(jnp.bfloat16)
    residual = jnp.concatenate([pick(relative, b) for b in order], axis=0)
    parts = jnp.stack([residual] + [line(residual, k) for k in range(1, lines)])
    parts, staged = lax.optimization_barrier((parts, staged))
    stream = jnp.concatenate([pick(parts, b) for b in order], axis=1)
    wide = stream.astype(jnp.float32)
    normed = (
        wide * lax.rsqrt(jnp.mean(wide * wide, axis=-1, keepdims=True) + 1e-05) * norm_gain
    ).astype(jnp.bfloat16)
    distant = near(normed)
    mate_rows = across(normed)
    mine_stream = lax.optimization_barrier(cut(wide, corner, half, 0) * 1.0)
    scale = scales(normed, *own_masks, router_weight)
    kept, sent = run_experts(normed, mate_rows, *staged)
    back = across(sent)

    def weigh(values, weights):
        weighted = (values * weights).reshape(lines, half, width)
        return weighted, weighted.astype(jnp.bfloat16)

    def slant(value, k):
        return lax.ppermute(value, "tok", [(t, t ^ (2 * k) ^ 1) for t in range(toks)])

    own_others = []
    weighted, low = weigh(kept + back.astype(jnp.float32), scale)
    total = pick(weighted, order[0])
    for k in range(1, lines):
        own_others.append(line(pick(low, order[k]), k))
    distant, _ = lax.optimization_barrier((distant, total))
    far_mates = across(distant)
    far_kept, far_sent = run_experts(distant, far_mates, *staged)
    far_scale = scales(distant, *far_masks, router_weight)
    _, far_low = weigh(far_kept + across(far_sent).astype(jnp.float32), far_scale)
    far_others = [slant(pick(far_low, order[k]), k) for k in reversed(range(lines))]
    for value in own_others + far_others:
        total = total + value.astype(jnp.float32)
    result = (mine_stream + total).astype(jnp.bfloat16)
    mate = across(result)
    low = jnp.where(first_side, result, mate)
    high = jnp.where(first_side, mate, result)
    return jnp.concatenate([low, high], axis=0)


def solution(mesh):
    return jax.shard_map(
        local,
        mesh=mesh,
        in_specs=(
            P(("grp", "tok"), None),
            P(("grp", "tok"), "side", None),
            P(("grp", "tok"), "side", None),
            P(("grp", "tok"), "side", None),
            P(("grp", "tok"), "side", None, None),
            P(("grp", "tok"), "side", None, None),
            P(("grp", "tok")),
            P("side", "tok"),
            P(),
            P(),
            P(None, ("tok", "side")),
            P(None, ("tok", "side")),
            P(("tok", "side"), None),
            P("grp", None),
        ),
        out_specs=P(("grp", "tok"), None),
        check_vma=False,
    )
```

```python
import math

import jax
import jax.numpy as jnp
from jax import lax
from jax.experimental import pallas as pl
from jax.experimental.pallas import tpu as pltpu
from jax.sharding import PartitionSpec as P


def attend(queries, key_new, value_new, cache_keys, cache_values, lengths):
    seq_count, head_count, head_width = queries.shape
    kv_count = key_new.shape[1]
    places = cache_keys.shape[2]
    scaling = 1.0 / math.sqrt(head_width)
    grouped = queries.reshape(seq_count, kv_count, head_count // kv_count, head_width)
    scores = (
        jnp.einsum("skgd,skpd->skgp", grouped, cache_keys, preferred_element_type=jnp.float32)
        * scaling
    )
    usable = jnp.arange(places, dtype=jnp.int32)[None, :] < lengths[:, None]
    scores = jnp.where(usable[:, None, None, :], scores, -jnp.inf)
    own_score = (
        jnp.einsum("skgd,skd->skg", grouped, key_new, preferred_element_type=jnp.float32) * scaling
    )
    top_score = jnp.maximum(jnp.max(scores, axis=-1), own_score)
    weights = jnp.exp(scores - top_score[..., None])
    own_weight = jnp.exp(own_score - top_score)
    totals = jnp.sum(weights, axis=-1) + own_weight
    prob_low = (weights / totals[..., None]).astype(jnp.bfloat16)
    own_low = (own_weight / totals).astype(jnp.bfloat16)
    mixture = jnp.einsum(
        "skgp,skpd->skgd", prob_low, cache_values, preferred_element_type=jnp.float32
    )
    mixture = (
        mixture
        + own_low.astype(jnp.float32)[..., None] * value_new.astype(jnp.float32)[:, :, None, :]
    )
    return mixture.astype(jnp.bfloat16).reshape(seq_count, head_count * head_width)


def scales(normed, picks, mine, router_weight):
    logits = jnp.dot(normed.astype(jnp.float32), router_weight, precision=lax.Precision.HIGHEST)
    chosen = jnp.sum(picks * logits[:, None, :], axis=-1)
    leading = jax.nn.sigmoid(chosen[:, 0] - chosen[:, 1])
    return (leading * mine[:, 0] + (1.0 - leading) * mine[:, 1])[:, None]


def cut(array, start, size, axis):
    return lax.dynamic_slice_in_dim(array, start, size, axis, allow_negative_indices=False)


def experts_kernel(own, other, gate, up_low, up_high, down, kept, sent, block, active):
    rows = own.shape[0]
    middle = up_low.shape[1]
    step = min(512, middle)
    block[:rows] = own[...]
    block[rows:] = other[...]
    for c in range(0, gate.shape[1], step):
        gated = jnp.dot(block[...], gate[:, c : c + step], preferred_element_type=jnp.float32)
        up, at = (up_low, c) if c < middle else (up_high, c - middle)
        upward = jnp.dot(block[...], up[:, at : at + step], preferred_element_type=jnp.float32)
        active[:, c : c + step] = (jax.nn.silu(gated) * upward).astype(jnp.bfloat16)
    for c in range(0, down.shape[1], 512):
        out = jnp.dot(active[...], down[:, c : c + 512], preferred_element_type=jnp.float32)
        kept[:, c : c + 512] = out[:rows]
        sent[:, c : c + 512] = out[rows:].astype(jnp.bfloat16)


def stage(weight, begin=0, count=None):
    shape = (weight.shape[0], count or weight.shape[1])

    def body(source, target):
        pltpu.sync_copy(source.at[:, pl.ds(begin, shape[1])], target)

    return pl.pallas_call(
        body,
        in_specs=[pl.BlockSpec(memory_space=pltpu.HBM)],
        out_specs=pl.BlockSpec(memory_space=pltpu.VMEM),
        out_shape=pltpu.VMEM(shape, weight.dtype),
        cost_estimate=pl.CostEstimate(
            flops=math.prod(shape) * 600,
            transcendentals=0,
            bytes_accessed=2 * math.prod(shape),
        ),
        compiler_params=pltpu.CompilerParams(vmem_limit_bytes=1 << 20),
        name="stage",
    )(pltpu.with_memory_space_constraint(weight, pltpu.HBM))


def run_experts(own, other, *weights):
    rows, width = own.shape
    size = weights[0].size
    fast = pl.BlockSpec(memory_space=pltpu.VMEM)
    return pl.pallas_call(
        experts_kernel,
        in_specs=[fast] * 6,
        out_specs=[fast] * 2,
        out_shape=[
            jax.ShapeDtypeStruct((rows, width), jnp.float32),
            jax.ShapeDtypeStruct((rows, width), jnp.bfloat16),
        ],
        scratch_shapes=[
            pltpu.VMEM((2 * rows, width), jnp.bfloat16),
            pltpu.VMEM((2 * rows, weights[0].shape[1]), jnp.bfloat16),
        ],
        cost_estimate=pl.CostEstimate(
            flops=3 * size * 600, transcendentals=0, bytes_accessed=4 * size
        ),
        compiler_params=pltpu.CompilerParams(vmem_limit_bytes=12 << 20),
        name="experts",
    )(own, other, *[pltpu.with_memory_space_constraint(w, pltpu.VMEM) for w in weights])


def pick(stack, index):
    return cut(stack, index, 1, 0).reshape(stack.shape[1:])


def local(
    hidden_in,
    queries,
    key_new,
    value_new,
    cache_keys,
    cache_values,
    lengths,
    out_weight,
    norm_gain,
    router_weight,
    gate_weight,
    up_weight,
    down_weight,
    routes,
):
    rows, width = hidden_in.shape
    toks = lax.axis_size("tok")
    sides = lax.axis_size("side")
    experts = router_weight.shape[1]
    lines = toks // 2
    half = rows // sides
    cols = out_weight.shape[1]
    span = out_weight.shape[0]
    tok = lax.axis_index("tok")
    side = lax.axis_index("side")
    first_swap = [(t, t ^ 1) for t in range(toks)]
    side_swap = [(0, 1), (1, 0)]

    def across(value):
        return lax.ppermute(value, "side", side_swap)

    def near(value):
        return lax.ppermute(value, "tok", first_swap)

    def line(value, k):
        return lax.ppermute(value, "tok", [(t, t ^ (2 * k)) for t in range(toks)])

    groups = lax.axis_size("grp")
    group = lax.axis_index("grp")
    level = tok // 2
    parity = tok % 2

    def over(value, k):
        return lax.ppermute(value, "grp", [(g, g ^ k) for g in range(groups)])

    shares = groups + 1 if span % (8 * (groups + 1)) == 0 else groups
    share = span // shares
    brought = near(cut(out_weight, group * share, share, 0))
    rest = [near(out_weight[groups * share :])] if shares > groups else []
    gathered = jnp.stack([brought] + [over(brought, k) for k in range(1, groups)])

    hidden_half = cut(hidden_in, side * half, half, 0)
    expert = tok // (toks // experts)
    expert_ids = jnp.arange(experts, dtype=jnp.int32)

    def masks(which):
        chosen = lax.dynamic_slice(
            routes.reshape(lines, 2, sides, half, -1),
            (0, which, side, 0, 0),
            (lines, 1, 1, half, routes.shape[1]),
            allow_negative_indices=False,
        ).reshape(lines * half, -1)
        picks = (chosen[:, :, None] == expert_ids[None, None, :]).astype(jnp.float32)
        return picks, (chosen == expert).astype(jnp.float32)

    own_masks, far_masks = masks(parity), masks(1 - parity)
    order = [level ^ b for b in range(lines)]
    starts = [b * (2 * cols) for b in order]
    shares_order = [group ^ b for b in range(groups)]
    even = parity == 0
    first_side = side == 0
    corner = level * half
    ahead = (own_masks, far_masks, order, starts, shares_order, even, first_side, corner, side)
    queries, ahead, away = lax.optimization_barrier((queries, ahead, 1 - side))
    own_masks, far_masks, order, starts, shares_order, even, first_side, corner, side = ahead
    attn_out = attend(queries, key_new, value_new, cache_keys, cache_values, lengths)
    up_half = up_weight.shape[1] // 2
    up_low = stage(up_weight, 0, up_half)
    up_high = stage(up_weight, up_half, up_half)
    down_staged = stage(down_weight)
    staged = [stage(gate_weight), up_low, up_high, down_staged]
    messages = []
    for k in range(lines):
        part = cut(hidden_half, starts[k], 2 * cols, 1)
        folds = span // (2 * cols)
        deep = half // folds
        extra = jnp.concatenate([part[i * deep : (i + 1) * deep] for i in range(folds)], axis=1)
        message = jnp.concatenate([attn_out, extra], axis=0)
        messages.append(message)
    sent_lines = {}
    for k in reversed(range(1, lines)):
        sent_lines[k] = line(messages[k], k)
    arrived = [messages[0]] + [sent_lines[k] for k in range(1, lines)]
    arrived, staged[:2] = lax.optimization_barrier((arrived, staged[:2]))
    blocks = jnp.concatenate([m[:rows] for m in arrived], axis=0)
    hidden_blocks = jnp.stack(
        [
            jnp.concatenate(
                [m[rows:, i * 2 * cols : (i + 1) * 2 * cols] for i in range(folds)], axis=0
            )
            for m in arrived
        ]
    )
    own_columns = jnp.dot(blocks, out_weight, preferred_element_type=jnp.float32)
    blocks, own_columns = lax.optimization_barrier((blocks, own_columns))
    far_weight = jnp.concatenate([pick(gathered, b) for b in shares_order] + rest, axis=0)
    far_columns = jnp.dot(blocks, far_weight, preferred_element_type=jnp.float32)
    columns = jnp.concatenate(
        [
            jnp.where(even, own_columns, far_columns),
            jnp.where(even, far_columns, own_columns),
        ],
        axis=1,
    ).reshape(lines, sides, half, 2 * cols)
    other = cut(columns, away, 1, 1).reshape(lines, half, 2 * cols)
    own = cut(columns, side, 1, 1).reshape(lines, half, 2 * cols)
    relative = (hidden_blocks.astype(jnp.float32) + (own + across(other))).astype(jnp.bfloat16)
    residual = jnp.concatenate([pick(relative, b) for b in order], axis=0)
    gathers = [line(residual, k) for k in range(1, lines)]
    parts = jnp.stack([residual] + gathers)
    parts, staged = lax.optimization_barrier((parts, staged))
    stream = jnp.concatenate([pick(parts, b) for b in order], axis=1)
    wide = stream.astype(jnp.float32)
    normed = (
        wide * lax.rsqrt(jnp.mean(wide * wide, axis=-1, keepdims=True) + 1e-05) * norm_gain
    ).astype(jnp.bfloat16)
    distant = near(normed)
    mate_rows = across(normed)
    mine_stream = lax.optimization_barrier(cut(wide, corner, half, 0) * 1.0)
    scale = scales(normed, *own_masks, router_weight)
    kept, sent = run_experts(normed, mate_rows, *staged)
    back = across(sent)

    def weigh(values, weights):
        weighted = (values * weights).reshape(lines, half, width)
        return weighted, weighted.astype(jnp.bfloat16)

    def slant(value, k):
        return lax.ppermute(value, "tok", [(t, t ^ (2 * k) ^ 1) for t in range(toks)])

    own_others = []
    weighted, low = weigh(kept + back.astype(jnp.float32), scale)
    total = pick(weighted, order[0])
    for k in range(1, lines):
        own_others.append(line(pick(low, order[k]), k))
    distant, _ = lax.optimization_barrier((distant, total))
    far_mates = across(distant)
    far_kept, far_sent = run_experts(distant, far_mates, *staged)
    far_scale = scales(distant, *far_masks, router_weight)
    _, far_low = weigh(far_kept + across(far_sent).astype(jnp.float32), far_scale)
    far_others = [slant(pick(far_low, order[k]), k) for k in reversed(range(lines))]
    for value in own_others + far_others:
        total = total + value.astype(jnp.float32)
    result = (mine_stream + total).astype(jnp.bfloat16)
    mate = across(result)
    low = jnp.where(first_side, result, mate)
    high = jnp.where(first_side, mate, result)
    return jnp.concatenate([low, high], axis=0)


def solution(mesh):
    return jax.shard_map(
        local,
        mesh=mesh,
        in_specs=(
            P(("grp", "tok"), None),
            P(("grp", "tok"), "side", None),
            P(("grp", "tok"), "side", None),
            P(("grp", "tok"), "side", None),
            P(("grp", "tok"), "side", None, None),
            P(("grp", "tok"), "side", None, None),
            P(("grp", "tok")),
            P("side", "tok"),
            P(),
            P(),
            P(None, ("tok", "side")),
            P(None, ("tok", "side")),
            P(("tok", "side"), None),
            P("grp", None),
        ),
        out_specs=P(("grp", "tok"), None),
        check_vma=False,
    )
```
